32 devices in a mesh: node: 32 (over z, y, x, core).
Axes of the slice: x: 2, y: 2, z: 4, core: 2. Of those that a mesh axis runs over, the one named last changes fastest.
Arguments:
- params: float32 [16384, 2048], P('node'), may hold values from -6 to 6
- public: float32 [16384, 2048], P('node'), may hold values from -4 to 4
- peer_public: float32 [16384, 2048], P('node'), may hold values from -8 to 8
- round_index: int32 [1], replicated, may hold values from 0 to 63
Outputs:
- params_new: float32 [16384, 2048], P('node')
- public_new: float32 [16384, 2048], P('node')
- peer_public_new: float32 [16384, 2048], P('node')
- consensus_gap: float32 [], replicated
The draws below stay inside these ranges and needn't reach their ends.
All inputs are finite; a program needn't handle non-finite values.
Results may differ from the reference program's by a relative error of at most 0.0003.
Values may be sent and summed in bfloat16 or wider, within the bound.
A program may use at most 128 MiB of HBM per device.

```python
import jax
import jax.numpy as jnp

D = 2048
ROWS = 512
BLOCK = 128
NODES = 32
N_NODE = 32


def lattice_pair(key):
    base_key = jax.random.fold_in(key, 7)
    keys = jax.random.split(base_key, 8)
    block_count = NODES * ROWS // BLOCK
    shape = (block_count, BLOCK, D)
    worker_factor = jax.random.uniform(keys[7], (NODES,), jnp.float32, 0.1, 1.0)
    block_worker = jnp.arange(block_count, dtype=jnp.int32) // (ROWS // BLOCK)
    block_factor = jnp.take(worker_factor, block_worker, axis=0)[:, None, None]
    public = jnp.clip(jax.random.normal(keys[0], shape, jnp.float32), -4.0, 4.0)
    scale = jnp.exp(jax.random.uniform(keys[1], (block_count, 1, D), jnp.float32, jnp.log(0.1), jnp.log(1.0)))
    offset = jax.random.uniform(keys[2], shape, jnp.float32, 0.1, 0.4)
    public = public * block_factor
    scale = scale.astype(jnp.bfloat16).astype(jnp.float32)
    level = jax.random.randint(keys[3], shape, -126, 127).astype(jnp.float32)
    sign_bits = jax.random.randint(keys[4], shape, 0, 2)
    signed_offset = jnp.where(sign_bits == 1, offset, -offset)
    value = level + signed_offset
    value = jnp.clip(value, -126.45, 126.45)
    pick = jax.random.randint(keys[5], (block_count, 1, D), 0, BLOCK)
    rows = jnp.arange(BLOCK, dtype=jnp.int32)[None, :, None]
    peak_sign = jnp.where(jax.random.randint(keys[6], (block_count, 1, D), 0, 2) == 1, 1.0, -1.0)
    delta = scale * value / 127.0
    delta = jnp.where(rows == pick, peak_sign * scale, delta)
    params = public + delta
    return (params.reshape(NODES * ROWS, D), public.reshape(NODES * ROWS, D))


def draw_params(key, part):
    return lattice_pair(key)[0]


def draw_public(key, part):
    return lattice_pair(key)[1]


def draw_peer_public(key, part):
    keys = jax.random.split(jax.random.fold_in(key, 11), 4)
    worker_ids = jnp.arange(NODES * ROWS, dtype=jnp.int32) // ROWS
    ramp_all = jnp.arange(NODES, dtype=jnp.float32) / jnp.float32(max(NODES - 1, 1))
    ramp_low = jax.random.uniform(keys[1], (), jnp.float32, 0.25, 0.5)
    ramp_high = jax.random.uniform(keys[2], (), jnp.float32, 1.0, 1.6)
    jitter = jnp.exp(jax.random.uniform(keys[3], (NODES,), jnp.float32, jnp.log(0.7), jnp.log(1.25)))
    base = jnp.clip(jax.random.normal(keys[0], (NODES * ROWS, D), jnp.float32), -4.0, 4.0)
    worker_factor = (ramp_low + (ramp_high - ramp_low) * ramp_all) * jitter
    row_factor = jnp.take(worker_factor, worker_ids, axis=0)
    return base * row_factor[:, None]


def setup_inputs(seed: int = 0) -> dict:
    splits = jax.random.split(jax.random.key(seed), 5)
    return {
        "params": draw_params(jax.random.fold_in(splits[4], 71), 0),
        "public": draw_public(jax.random.fold_in(splits[4], 71), 0),
        "peer_public": draw_peer_public(jax.random.fold_in(splits[4], 71), 0),
        "round_index": jax.random.randint(splits[3], (1,), 0, 64).astype(jnp.int32),
    }


def reference(params, public, peer_public, round_index):
    bit_count = N_NODE.bit_length() - 1
    chosen_bit = round_index[0] % bit_count
    offset = jnp.left_shift(jnp.int32(1), chosen_bit.astype(jnp.int32))
    node_ids = jnp.arange(NODES, dtype=jnp.int32)
    partner = jnp.bitwise_xor(node_ids, offset).astype(jnp.int32)
    difference = (params - public).reshape(NODES, ROWS // BLOCK, BLOCK, D)
    block_peak = jnp.max(jnp.abs(difference), axis=2) + 1e-6
    block_scale = block_peak.astype(jnp.bfloat16)
    wide_scale = block_scale.astype(jnp.float32)[:, :, None, :]
    coded = jnp.floor((difference / wide_scale) * 127.0 + 0.5).astype(jnp.bfloat16)
    own_delta = (coded.astype(jnp.float32) * wide_scale) / 127.0
    partner_delta = jnp.take(own_delta, partner, axis=0)
    own_delta = own_delta.reshape(NODES * ROWS, D)
    partner_delta = partner_delta.reshape(NODES * ROWS, D)
    public_new = public + own_delta
    peer_public_new = peer_public + partner_delta
    params_new = params + 0.4 * (peer_public_new - public_new)
    distance = params_new - public_new
    consensus_gap = jnp.sum(distance * distance) / jnp.float32(NODES * ROWS * D)
    return params_new, public_new, peer_public_new, consensus_gap
```

```python
from functools import partial

import jax
import jax.numpy as jnp
from jax import lax
from jax.experimental import pallas as pl
from jax.experimental.pallas import tpu as pltpu
from jax.sharding import PartitionSpec as P

BLOCK = 128
MIX = 0.4
WIDE = 512
STRIP = 128
FIRST = (8, 16)
MESH = pl.DeviceIdType.MESH
ANY = pl.BlockSpec(memory_space=pl.ANY)
VMEM = pl.BlockSpec(memory_space=pltpu.VMEM)
HBM = pl.BlockSpec(memory_space=pltpu.HBM)


def place(k, col_count):
    across = col_count // WIDE
    rows = pl.ds(pl.multiple_of(k // across * BLOCK, BLOCK), BLOCK)
    return rows, pl.multiple_of(k % across * WIDE, WIDE)


def area(k, col_count):
    rows, first = place(k, col_count)
    return rows, pl.ds(first, WIDE)


def cut(chunks):
    first, second = (chunks * f // 16 for f in FIRST)
    return first + (second - first) * lax.rem(lax.axis_index("node"), 2)


class Pair:
    def __init__(self, bit, send_sem, recv_sem):
        self.me = lax.axis_index("node")
        self.mask = 1 << bit
        self.upper = self.me // self.mask % 2
        self.other = self.me + self.mask - 2 * self.mask * self.upper
        self.send_sem, self.recv_sem = send_sem, recv_sem

    def tell(self, sem):
        pl.semaphore_signal(sem, inc=1, device_id=(self.other,), device_id_type=MESH)

    def copy(self, source, target, part, k):
        return pltpu.make_async_remote_copy(
            src_ref=source,
            dst_ref=target,
            send_sem=self.send_sem.at[part, k],
            recv_sem=self.recv_sem.at[part, k],
            device_id=(self.other,),
            device_id_type=MESH,
        )


def merge(pair, k, slot, total, got_coded, got_scale, mine, shared, peer, mine_new, peer_new, spot):
    rows, first = place(k, shared.shape[1])
    for strip in range(0, WIDE, STRIP):
        columns = pl.ds(pl.multiple_of(first + strip, STRIP), STRIP)
        factor = got_scale[k, :, strip : strip + STRIP].astype(jnp.float32) * (1.0 / 127.0)
        level = got_coded[slot, :, strip : strip + STRIP].astype(jnp.float32)
        theirs = peer[rows, columns] + level * factor
        public_new = shared[rows, columns]
        params_new = mine[rows, columns] + MIX * (theirs - public_new)
        target = spot(rows, columns, strip)
        peer_new[target] = theirs
        mine_new[target] = params_new
        distance = params_new - public_new
        total = total + jnp.sum(distance * distance, axis=0, keepdims=True)
    return total


def greet_pairs(pair, n, barrier):
    half, mask = n // 2, pair.mask
    mine = pair.me // (2 * mask) * mask + pair.me % mask

    @pl.when(pair.upper == 0)
    def _():
        def greet(k, carry):
            t = lax.rem(mine + k, half)
            low = t // mask * (2 * mask) + t % mask
            pl.semaphore_signal(barrier, inc=1, device_id=(low,), device_id_type=MESH)
            return carry

        lax.fori_loop(1, half, greet, 0)


def hear_pairs(pair, n, barrier, all_in):
    @pl.when(pair.upper == 0)
    def _():
        pl.semaphore_wait(barrier, n // 2 - 1)
        pair.tell(all_in)


def add_rows(pair, part, rows_in, row_send, row_recv, all_in):
    n = rows_in.shape[0]

    @pl.when(pair.upper == 1)
    def _():
        pl.semaphore_wait(all_in, 1)

    def row_copy(source, place, target):
        return pltpu.make_async_remote_copy(
            src_ref=source,
            dst_ref=place,
            send_sem=row_send,
            recv_sem=row_recv,
            device_id=(target,),
            device_id_type=MESH,
        )

    def send_row(k, carry):
        row_copy(part, rows_in.at[pair.me], lax.rem(pair.me + k, n)).start()
        return carry

    lax.fori_loop(1, n, send_row, 0)
    rows_in[pair.me] = part[...]
    rest = rows_in.at[pl.ds(1, n - 1)]
    row_copy(rest, rest, pair.other).wait()
    return jnp.sum(jnp.sum(rows_in[...], axis=0), axis=1, keepdims=True)


def first_kernel(bit, lead, last, inverse, params_hbm, public_hbm, peer_hbm, *refs):
    mine, shared, peer = refs[:3]
    if last:
        gap_out, coded, got_coded, got_scale = refs[3:7]
        scale, load_sem, peer_sem, send_sem, recv_sem = refs[7:12]
        ready, all_in, part, rows_in, row_send, row_recv = refs[12:]
    else:
        coded, scale_out, part, got_coded, got_scale = refs[3:8]
        scale, load_sem, peer_sem, send_sem, recv_sem = refs[8:]
    chunks = coded.shape[0]
    cols = shared.shape[1]
    stop = chunks if last else cut(chunks)
    pair = Pair(bit, send_sem, recv_sem)
    barrier = pltpu.get_barrier_semaphore()

    if last:

        @pl.when(pair.upper == 0)
        def _():
            pair.tell(barrier)
    else:
        pair.tell(barrier)

    def load(k, source, target, sem):
        here = area(k, cols)
        return pltpu.make_async_copy(source.at[here], target.at[here], sem)

    def send_coded(k):
        return pair.copy(coded.at[k], got_coded.at[k], 0, k)

    def send_scale(k):
        return pair.copy(scale.at[k], got_scale.at[k], 1, k)

    def send_rest():
        rest = pl.ds(lead, chunks - lead)
        return pair.copy(scale.at[rest], got_scale.at[rest], 1, lead)

    def begin(k, carry):
        load(k, params_hbm, mine, load_sem.at[0, k]).start()
        load(k, public_hbm, shared, load_sem.at[1, k]).start()
        return carry

    lax.fori_loop(0, chunks, begin, 0)

    if last:

        @pl.when(pair.upper == 1)
        def _():
            pl.semaphore_wait(barrier, 1)
            pair.tell(ready)

    def encode(k, carry):
        rows, first = place(k, cols)
        load(k, params_hbm, mine, load_sem.at[0, k]).wait()
        load(k, public_hbm, shared, load_sem.at[1, k]).wait()
        for strip in range(0, WIDE, STRIP):
            columns = pl.ds(pl.multiple_of(first + strip, STRIP), STRIP)
            difference = mine[rows, columns] - shared[rows, columns]
            peak = jnp.max(jnp.abs(difference), axis=0, keepdims=True) + 1e-06
            rounded = peak.astype(jnp.bfloat16)
            scale[k, :, strip : strip + STRIP] = rounded
            wide = rounded.astype(jnp.float32)
            level = jnp.floor(difference / wide * 127.0 + 0.5)
            coded[k, :, strip : strip + STRIP] = level.astype(jnp.bfloat16)
        for strip in range(0, WIDE, STRIP):
            columns = pl.ds(pl.multiple_of(first + strip, STRIP), STRIP)
            factor = scale[k, :, strip : strip + STRIP].astype(jnp.float32) * (1.0 / 127.0)
            level = coded[k, :, strip : strip + STRIP].astype(jnp.float32)
            shared[rows, columns] = shared[rows, columns] + level * factor

        @pl.when(k == 0)
        def _():
            if last:

                @pl.when(pair.upper == 0)
                def _():
                    pl.semaphore_wait(ready, 1)
            else:
                pl.semaphore_wait(barrier, 1)

        @pl.when(k < lead)
        def _():
            send_scale(k).start()
            send_coded(k).start()

        load(k, peer_hbm, peer, peer_sem.at[k]).start()
        return carry

    lax.fori_loop(0, chunks, encode, 0)

    if lead < chunks:
        send_rest().start()

        def send_more(k, carry):
            send_coded(k).start()
            return carry

        lax.fori_loop(lead, stop, send_more, 0)

    if last:
        greet_pairs(pair, rows_in.shape[0], barrier)

    def combine(k, total):
        load(k, peer_hbm, peer, peer_sem.at[k]).wait()
        if last:

            @pl.when(k == chunks - 1)
            def _():
                hear_pairs(pair, rows_in.shape[0], barrier, all_in)

        @pl.when(k < lead)
        def _():
            send_scale(k).wait_recv()

        if lead < chunks:

            @pl.when(k == lead)
            def _():
                send_rest().wait_recv()

        send_coded(k).wait_recv()
        return merge(
            pair, k, k, total, got_coded, got_scale, mine, shared, peer, mine, peer,
            lambda rows, columns, strip: (rows, columns),
        )

    part[...] = lax.fori_loop(0, stop, combine, jnp.zeros((1, STRIP), jnp.float32))

    def drain(k, carry):
        send_coded(k).wait_send()

        @pl.when(k < lead)
        def _():
            send_scale(k).wait_send()

        return carry

    def drain_all():
        lax.fori_loop(0, stop, drain, 0)
        if lead < chunks:
            send_rest().wait_send()

    if last:
        total = add_rows(pair, part, rows_in, row_send, row_recv, all_in)
        drain_all()
        gap_out[...] = jnp.broadcast_to(total * inverse, gap_out.shape)
    else:

        def land(k, carry):
            load(k, peer_hbm, peer, peer_sem.at[k]).wait()
            return carry

        lax.fori_loop(stop, chunks, land, 0)
        scale_out[...] = got_scale[...]
        drain_all()


def last_kernel(bit, inverse, mine, shared, peer, coded, got_scale, part_in, *refs):
    mine_new, peer_new, gap_out, got_coded, send_sem, recv_sem = refs[:6]
    ready, all_in, part, rows_in, row_send, row_recv = refs[6:]
    chunks = coded.shape[0]
    start = cut(chunks)
    pair = Pair(bit, send_sem, recv_sem)
    n = rows_in.shape[0]
    barrier = pltpu.get_barrier_semaphore()

    @pl.when(pair.upper == 0)
    def _():
        pair.tell(barrier)

    @pl.when(pair.upper == 1)
    def _():
        pl.semaphore_wait(barrier, 1)
        pair.tell(ready)

    @pl.when(pair.upper == 0)
    def _():
        pl.semaphore_wait(ready, 1)

    def send_coded(k):
        return pair.copy(coded.at[k], got_coded.at[k - start], 0, k)

    def send(k, carry):
        send_coded(k).start()
        return carry

    lax.fori_loop(start, chunks, send, 0)
    greet_pairs(pair, n, barrier)

    @pl.when(start == chunks)
    def _():
        hear_pairs(pair, n, barrier, all_in)

    def combine(k, total):
        @pl.when(k == chunks - 1)
        def _():
            hear_pairs(pair, n, barrier, all_in)

        send_coded(k).wait_recv()
        slot = k - start
        return merge(
            pair, k, slot, total, got_coded, got_scale, mine, shared, peer, mine_new, peer_new,
            lambda rows, columns, strip: (slot, slice(None), slice(strip, strip + STRIP)),
        )

    part[...] = lax.fori_loop(start, chunks, combine, part_in[...])
    total = add_rows(pair, part, rows_in, row_send, row_recv, all_in)

    def drain(k, carry):
        send_coded(k).wait_send()
        return carry

    lax.fori_loop(start, chunks, drain, 0)
    gap_out[...] = jnp.broadcast_to(total * inverse, gap_out.shape)


def whole_store_kernel(*refs):
    sources, gap, targets, sem, one = refs[:3], refs[3], refs[4:8], refs[8], refs[9]
    one[...] = gap[:, :1]
    pairs = zip((one, *sources), (targets[3], *targets[:3]))
    copies = [pltpu.make_async_copy(a, b, sem.at[i]) for i, (a, b) in enumerate(pairs)]
    for copy in copies:
        copy.start()
    for copy in copies:
        copy.wait()


def early_store_kernel(chunks, mine, shared, peer, part, mine_hbm, shared_hbm, peer_hbm, part_out, sem, shared_sem):
    stop = cut(chunks)
    cols = shared.shape[1]

    def copies(k):
        here = area(k, cols)
        return [
            pltpu.make_async_copy(a.at[here], b.at[here], sem.at[i, k])
            for i, (a, b) in enumerate(((mine, mine_hbm), (peer, peer_hbm)))
        ]

    whole = pltpu.make_async_copy(shared, shared_hbm, shared_sem)
    whole.start()

    def start(k, carry):
        for copy in copies(k):
            copy.start()
        return carry

    def wait(k, carry):
        for copy in copies(k):
            copy.wait()
        return carry

    lax.fori_loop(0, stop, start, 0)
    part_out[...] = part[...]
    whole.wait()
    lax.fori_loop(0, stop, wait, 0)


def late_store_kernel(chunks, mine, peer, gap, mine_old, peer_old, mine_hbm, peer_hbm, gap_hbm, sem, gap_sem, one):
    first = cut(chunks)
    cols = mine_hbm.shape[1]

    def copies(k):
        here = area(k, cols)
        return [
            pltpu.make_async_copy(a.at[k - first], b.at[here], sem.at[i, k])
            for i, (a, b) in enumerate(((mine, mine_hbm), (peer, peer_hbm)))
        ]

    one[...] = gap[:, :1]
    small = pltpu.make_async_copy(one, gap_hbm, gap_sem)
    small.start()

    def start(k, carry):
        for copy in copies(k):
            copy.start()
        return carry

    def wait(k, carry):
        for copy in copies(k):
            copy.wait()
        return carry

    lax.fori_loop(first, chunks, start, 0)
    small.wait()
    lax.fori_loop(first, chunks, wait, 0)


def shape(*dims):
    return pltpu.HBM(dims, jnp.float32)


def params_of(limit, collective_id=None):
    if collective_id is None:
        return pltpu.CompilerParams(vmem_limit_bytes=limit)
    return pltpu.CompilerParams(
        collective_id=collective_id, has_side_effects=True, vmem_limit_bytes=limit
    )


def cost(array, passes):
    return pl.CostEstimate(flops=passes * array.size, bytes_accessed=passes * array.size, transcendentals=0)


def row_scratch(n):
    return [
        pltpu.SemaphoreType.REGULAR,
        pltpu.SemaphoreType.REGULAR,
        pltpu.VMEM((1, STRIP), jnp.float32),
        pltpu.VMEM((n, 1, STRIP), jnp.float32),
        pltpu.SemaphoreType.DMA,
        pltpu.SemaphoreType.DMA,
    ]


def open_round(bit, last, params, public, peer_public):
    rows, cols = params.shape
    chunks = rows // BLOCK * (cols // WIDE)
    n = lax.axis_size("node")
    lead = chunks if last else min(2, chunks)
    full = pltpu.VMEM(params.shape, jnp.float32)
    levels = (chunks, BLOCK, WIDE)
    scales = (chunks, 1, WIDE)
    sems = [pltpu.SemaphoreType.DMA((2, chunks))] + [pltpu.SemaphoreType.DMA((chunks,))]
    sems += [pltpu.SemaphoreType.DMA((2, chunks))] * 2
    out = [full, full, full]
    scratch = [pltpu.VMEM(levels, jnp.bfloat16), pltpu.VMEM(scales, jnp.bfloat16), pltpu.VMEM(scales, jnp.bfloat16)]
    if last:
        out += [pltpu.VMEM((1, STRIP), jnp.float32)]
        scratch = [pltpu.VMEM(levels, jnp.bfloat16)] + scratch + sems + row_scratch(n)
    else:
        out += [pltpu.VMEM(levels, jnp.bfloat16), pltpu.VMEM(scales, jnp.bfloat16), pltpu.VMEM((1, STRIP), jnp.float32)]
        scratch = scratch + sems
    return pl.pallas_call(
        partial(first_kernel, bit, lead, last, 1.0 / (n * rows * cols)),
        in_specs=[ANY] * 3,
        out_specs=[VMEM] * len(out),
        out_shape=out,
        scratch_shapes=scratch,
        cost_estimate=cost(params, 30),
        compiler_params=params_of(24 << 20, 2 * bit + 1),
    )(params, public, peer_public)


def close_round(bit, chunks, *arrays):
    rows, cols = arrays[0].shape
    n = lax.axis_size("node")
    rest = chunks - min(chunks * f // 16 for f in FIRST)
    tail = pltpu.VMEM((rest, BLOCK, WIDE), jnp.float32)
    return pl.pallas_call(
        partial(last_kernel, bit, 1.0 / (n * rows * cols)),
        in_specs=[VMEM] * 6,
        out_specs=[VMEM] * 3,
        out_shape=[tail, tail, pltpu.VMEM((1, STRIP), jnp.float32)],
        scratch_shapes=[
            pltpu.VMEM((rest, BLOCK, WIDE), jnp.bfloat16),
            pltpu.SemaphoreType.DMA((1, chunks)),
            pltpu.SemaphoreType.DMA((1, chunks)),
        ]
        + row_scratch(n),
        cost_estimate=cost(arrays[0], 10),
        compiler_params=params_of(8 << 20, 2 * bit + 2),
    )(*arrays)


def store_all(*arrays):
    return pl.pallas_call(
        whole_store_kernel,
        in_specs=[VMEM] * 4,
        out_specs=[HBM] * 4,
        out_shape=[shape(*a.shape) for a in arrays[:3]] + [shape(1, 1)],
        scratch_shapes=[pltpu.SemaphoreType.DMA((4,)), pltpu.VMEM((1, 1), jnp.float32)],
        compiler_params=params_of(1 << 20),
    )(*arrays)


def store_early(chunks, mine, shared, peer, part):
    return pl.pallas_call(
        partial(early_store_kernel, chunks),
        in_specs=[VMEM] * 4,
        out_specs=[HBM] * 3 + [VMEM],
        out_shape=[shape(*mine.shape)] * 3 + [pltpu.VMEM(part.shape, jnp.float32)],
        scratch_shapes=[pltpu.SemaphoreType.DMA((2, chunks)), pltpu.SemaphoreType.DMA],
        compiler_params=params_of(1 << 20),
    )(mine, shared, peer, part)


def store_late(chunks, mine, peer, gap, mine_hbm, peer_hbm):
    return pl.pallas_call(
        partial(late_store_kernel, chunks),
        in_specs=[VMEM] * 3 + [HBM] * 2,
        out_specs=[HBM] * 3,
        out_shape=[shape(*mine_hbm.shape)] * 2 + [shape(1, 1)],
        input_output_aliases={3: 0, 4: 1},
        scratch_shapes=[
            pltpu.SemaphoreType.DMA((2, chunks)),
            pltpu.SemaphoreType.DMA,
            pltpu.VMEM((1, 1), jnp.float32),
        ],
        compiler_params=params_of(1 << 20),
    )(mine, peer, gap, mine_hbm, peer_hbm)


def round_of(bit, params, public, peer_public):
    if bit == 0:
        return store_all(*open_round(bit, True, params, public, peer_public))
    mine, shared, peer, coded, scale, part = open_round(bit, False, params, public, peer_public)
    chunks = coded.shape[0]
    params_new, public_new, peer_new, part = store_early(chunks, mine, shared, peer, part)
    mine, peer, gap = close_round(bit, chunks, mine, shared, peer, coded, scale, part)
    params_new, peer_new, gap = store_late(chunks, mine, peer, gap, params_new, peer_new)
    return params_new, public_new, peer_new, gap


def shards(params, public, peer_public, round_index):
    n = lax.axis_size("node")
    bit_count = n.bit_length() - 1
    chosen_bit = lax.rem(round_index[0], jnp.int32(bit_count))
    branches = [partial(round_of, bit) for bit in range(bit_count)]
    params_new, public_new, peer_new, gap = lax.switch(
        chosen_bit, branches, params, public, peer_public
    )
    return (params_new, public_new, peer_new, gap[0, 0])


def solution(mesh):
    in_specs = (P("node", None), P("node", None), P("node", None), P())
    out_specs = (P("node", None), P("node", None), P("node", None), P())
    return jax.shard_map(shards, mesh=mesh, in_specs=in_specs, out_specs=out_specs, check_vma=False)
```

```python
from functools import partial

import jax
import jax.numpy as jnp
from jax import lax
from jax.experimental import pallas as pl
from jax.experimental.pallas import tpu as pltpu
from jax.sharding import PartitionSpec as P

BLOCK = 128
MIX = 0.4
WIDE = 512
STRIP = 128
FIRST = ((8, 16), (16, 10))
EARLY = ((8, 10), (12, 10))
MESH = pl.DeviceIdType.MESH
ANY = pl.BlockSpec(memory_space=pl.ANY)
VMEM = pl.BlockSpec(memory_space=pltpu.VMEM)
HBM = pl.BlockSpec(memory_space=pltpu.HBM)


def place(k, col_count):
    across = col_count // WIDE
    rows = pl.ds(pl.multiple_of(k // across * BLOCK, BLOCK), BLOCK)
    return rows, pl.multiple_of(k % across * WIDE, WIDE)


def area(k, col_count):
    rows, first = place(k, col_count)
    return rows, pl.ds(first, WIDE)


def by_place(bit, table, chunks):
    me, mask = lax.axis_index("node"), 1 << bit
    rows = [[chunks * sixteenths // 16 for sixteenths in row] for row in table]
    usual, other = (first + (second - first) * (me % 2) for first, second in rows)
    if 2 * mask == lax.axis_size("node"):
        return other
    low = me - mask * (me // mask % 2)
    return other + (usual - other) * jnp.minimum(low // 2, 1)


def cut(bit, chunks):
    return by_place(bit, FIRST, chunks)


class Pair:
    def __init__(self, bit, send_sem, recv_sem):
        self.me = lax.axis_index("node")
        self.mask = 1 << bit
        self.upper = self.me // self.mask % 2
        self.other = self.me + self.mask - 2 * self.mask * self.upper
        self.send_sem, self.recv_sem = send_sem, recv_sem

    def tell(self, sem):
        pl.semaphore_signal(sem, inc=1, device_id=(self.other,), device_id_type=MESH)

    def copy(self, source, target, part, k):
        return pltpu.make_async_remote_copy(
            src_ref=source,
            dst_ref=target,
            send_sem=self.send_sem.at[part, k],
            recv_sem=self.recv_sem.at[part, k],
            device_id=(self.other,),
            device_id_type=MESH,
        )


def merge(k, slot, total, got_coded, got_scale, mine, shared, peer, mine_new, peer_new, spot, before=None):
    rows, first = place(k, shared.shape[1])
    for strip in range(0, WIDE, STRIP):
        if before is not None:
            before(strip)
        columns = pl.ds(pl.multiple_of(first + strip, STRIP), STRIP)
        both = got_scale[k // 2, :, strip : strip + STRIP].astype(jnp.float32) * (1.0 / 127.0)
        factor = jnp.where(k % 2 == 0, both[:1], both[1:])
        level = got_coded[slot, :, strip : strip + STRIP].astype(jnp.float32)
        theirs = peer[rows, columns] + level * factor
        public_new = shared[rows, columns]
        params_new = mine[rows, columns] + MIX * (theirs - public_new)
        target = spot(rows, columns, strip)
        peer_new[target] = theirs
        mine_new[target] = params_new
        distance = params_new - public_new
        total = total + jnp.sum(distance * distance, axis=0, keepdims=True)
    return total


def greet_pairs(pair, n, barrier):
    half, mask = n // 2, pair.mask
    mine = pair.me // (2 * mask) * mask + pair.me % mask

    def greet(k, carry):
        t = lax.rem(mine + k, half)
        low = t // mask * (2 * mask) + t % mask
        pl.semaphore_signal(barrier, inc=1, device_id=(low,), device_id_type=MESH)
        return carry

    lax.fori_loop(1, half, greet, 0)


def hear_pairs(pair, n, barrier, all_in):
    @pl.when(pair.upper == 0)
    def _():
        pl.semaphore_wait(barrier, n - 2)
        pair.tell(all_in)


def add_rows(pair, part, rows_in, row_send, row_recv, all_in, drain):
    n = rows_in.shape[0]

    @pl.when(pair.upper == 1)
    def _():
        pl.semaphore_wait(all_in, 1)

    def row_copy(source, place, target):
        return pltpu.make_async_remote_copy(
            src_ref=source,
            dst_ref=place,
            send_sem=row_send,
            recv_sem=row_recv,
            device_id=(target,),
            device_id_type=MESH,
        )

    def send_row(k, carry):
        row_copy(part, rows_in.at[pair.me], lax.rem(pair.me + k, n)).start()
        return carry

    lax.fori_loop(1, n, send_row, 0)
    rows_in[pair.me] = part[...]
    drain()
    rest = rows_in.at[pl.ds(1, n - 1)]
    row_copy(rest, rest, pair.other).wait()
    return jnp.sum(jnp.sum(rows_in[...], axis=0), axis=1, keepdims=True)


def first_kernel(bit, lead, last, inverse, params_hbm, public_hbm, peer_hbm, *refs):
    mine, shared, peer = refs[:3]
    if last:
        gap_out, coded, got_coded, got_scale = refs[3:7]
        scale, load_sem, strip_sem, peer_sem, send_sem, recv_sem = refs[7:13]
        ready, all_in, part, rows_in, row_send, row_recv = refs[13:]
    else:
        coded, scale_out, part, got_coded, got_scale = refs[3:8]
        scale, load_sem, strip_sem, peer_sem, send_sem, recv_sem = refs[8:]
    chunks = coded.shape[0]
    cols = shared.shape[1]
    stop = chunks if last else cut(bit, chunks)
    pair = Pair(bit, send_sem, recv_sem)
    barrier = pltpu.get_barrier_semaphore()

    if last:

        @pl.when(pair.upper == 0)
        def _():
            pair.tell(barrier)

        greet_pairs(pair, rows_in.shape[0], barrier)
    else:
        pair.tell(barrier)

    def load(k, source, target, sem):
        here = area(k, cols)
        return pltpu.make_async_copy(source.at[here], target.at[here], sem)

    def send_coded(k):
        return pair.copy(coded.at[k], got_coded.at[k], 0, k)

    def send_scale(i):
        return pair.copy(scale.at[i], got_scale.at[i], 1, i)

    def send_rest():
        rest = pl.ds(lead // 2, (chunks - lead) // 2)
        return pair.copy(scale.at[rest], got_scale.at[rest], 1, lead // 2)

    def load_strip(i, strip):
        here = (pl.ds(0, BLOCK), pl.ds(strip, STRIP))
        source, target = ((params_hbm, mine), (public_hbm, shared))[i]
        return pltpu.make_async_copy(source.at[here], target.at[here], strip_sem.at[i, strip // STRIP])

    def send_strip(strip):
        here = (0, slice(None), pl.ds(strip, STRIP))
        return pair.copy(coded.at[here], got_coded.at[here], 0, 0)

    for strip in range(0, WIDE, STRIP):
        for i in range(2):
            load_strip(i, strip).start()

    def begin(k, carry):
        load(k, params_hbm, mine, load_sem.at[0, k]).start()
        load(k, public_hbm, shared, load_sem.at[1, k]).start()
        return carry

    lax.fori_loop(1, chunks, begin, 0)

    if last:

        @pl.when(pair.upper == 1)
        def _():
            pl.semaphore_wait(barrier, 1)
            pair.tell(ready)

    def met():
        if last:

            @pl.when(pair.upper == 0)
            def _():
                pl.semaphore_wait(ready, 1)
        else:
            pl.semaphore_wait(barrier, 1)

    def encode(k, opening):
        rows, first = place(k, cols)
        if not opening:
            load(k, params_hbm, mine, load_sem.at[0, k]).wait()
            load(k, public_hbm, shared, load_sem.at[1, k]).wait()
        scales = []
        for strip in range(0, WIDE, STRIP):
            if opening:
                for i in range(2):
                    load_strip(i, strip).wait()
            columns = pl.ds(pl.multiple_of(first + strip, STRIP), STRIP)
            difference = mine[rows, columns] - shared[rows, columns]
            peak = jnp.max(jnp.abs(difference), axis=0, keepdims=True) + 1e-06
            wide = peak.astype(jnp.bfloat16).astype(jnp.float32)
            level = jnp.floor(difference / wide * 127.0 + 0.5)
            coded[k, :, strip : strip + STRIP] = level.astype(jnp.bfloat16)
            if opening:
                if strip == 0:
                    met()
                send_strip(strip).start()
            scales.append(wide)
        for strip, wide in zip(range(0, WIDE, STRIP), scales):
            columns = pl.ds(pl.multiple_of(first + strip, STRIP), STRIP)
            level = coded[k, :, strip : strip + STRIP].astype(jnp.float32)
            shared[rows, columns] = shared[rows, columns] + level * (wide * (1.0 / 127.0))
        return scales

    def encode_two(i, opening):
        k = 2 * i
        even = encode(k, opening)
        if not opening:

            @pl.when(k < lead)
            def _():
                send_coded(k).start()

        odd = encode(k + 1, False)
        first_row = lax.broadcasted_iota(jnp.int32, (2, STRIP), 0) == 0
        for strip, a, b in zip(range(0, WIDE, STRIP), even, odd):
            scale[i, :, strip : strip + STRIP] = jnp.where(first_row, a, b).astype(jnp.bfloat16)

        @pl.when(k < lead)
        def _():
            send_scale(i).start()
            send_coded(k + 1).start()

        for h in range(2):
            load(k + h, peer_hbm, peer, peer_sem.at[k + h]).start()

    def encode_later(i, carry):
        encode_two(i, False)
        return carry

    encode_two(0, True)
    lax.fori_loop(1, chunks // 2, encode_later, 0)

    if lead < chunks:
        send_rest().start()

        def send_more(k, carry):
            send_coded(k).start()
            return carry

        lax.fori_loop(lead, stop, send_more, 0)

    def combine(k, total):
        load(k, peer_hbm, peer, peer_sem.at[k]).wait()
        if last:

            @pl.when(k == chunks - 1)
            def _():
                hear_pairs(pair, rows_in.shape[0], barrier, all_in)

        @pl.when((k < lead) & (k % 2 == 0))
        def _():
            send_scale(k // 2).wait_recv()

        if lead < chunks:

            @pl.when(k == lead)
            def _():
                send_rest().wait_recv()

        send_coded(k).wait_recv()
        return merge(
            k, k, total, got_coded, got_scale, mine, shared, peer, mine, peer,
            lambda rows, columns, strip: (rows, columns),
        )

    part[...] = lax.fori_loop(0, stop, combine, jnp.zeros((1, STRIP), jnp.float32))

    def drain(k, carry):
        send_coded(k).wait_send()

        @pl.when((k < lead) & (k % 2 == 0))
        def _():
            send_scale(k // 2).wait_send()

        return carry

    def drain_all():
        lax.fori_loop(0, stop, drain, 0)
        if lead < chunks:
            send_rest().wait_send()

    if last:
        total = add_rows(pair, part, rows_in, row_send, row_recv, all_in, drain_all)
        gap_out[...] = jnp.broadcast_to(total * inverse, gap_out.shape)
    else:

        def land(k, carry):
            load(k, peer_hbm, peer, peer_sem.at[k]).wait()
            return carry

        lax.fori_loop(stop, chunks, land, 0)
        scale_out[...] = got_scale[...]
        drain_all()


def last_kernel(bit, inverse, mine, shared, peer, coded, got_scale, part_in, *refs):
    mine_new, peer_new, gap_out, got_coded, send_sem, recv_sem = refs[:6]
    ready, all_in, part, rows_in, row_send, row_recv = refs[6:]
    chunks = coded.shape[0]
    start = cut(bit, chunks)
    pair = Pair(bit, send_sem, recv_sem)
    n = rows_in.shape[0]
    barrier = pltpu.get_barrier_semaphore()

    @pl.when(pair.upper == 0)
    def _():
        pair.tell(barrier)

    greet_pairs(pair, n, barrier)

    @pl.when(pair.upper == 1)
    def _():
        pl.semaphore_wait(barrier, 1)
        pair.tell(ready)

    @pl.when(pair.upper == 0)
    def _():
        pl.semaphore_wait(ready, 1)

    def send_coded(k):
        return pair.copy(coded.at[k], got_coded.at[k - start], 0, k)

    end = chunks - 1

    def send_strip(strip):
        columns = pl.ds(strip, STRIP)
        source, target = coded.at[end, :, columns], got_coded.at[end - start, :, columns]
        return pair.copy(source, target, 1, strip // STRIP)

    strips = range(0, WIDE, STRIP)

    def send(k, carry):
        send_coded(k).start()
        return carry

    lax.fori_loop(start, end, send, 0)

    @pl.when(start < chunks)
    def _():
        for strip in strips:
            send_strip(strip).start()

    def combine(k, total, before=None):
        slot = k - start
        return merge(
            k, slot, total, got_coded, got_scale, mine, shared, peer, mine_new, peer_new,
            lambda rows, columns, strip: (slot, slice(None), slice(strip, strip + STRIP)), before
        )

    def take(k, total):
        send_coded(k).wait_recv()
        return combine(k, total)

    part[...] = lax.fori_loop(start, end, take, part_in[...])
    hear_pairs(pair, n, barrier, all_in)

    @pl.when(start < chunks)
    def _():
        part[...] = combine(end, part[...], lambda strip: send_strip(strip).wait_recv())

    def drain(k, carry):
        send_coded(k).wait_send()
        return carry

    def drain_all():
        lax.fori_loop(start, end, drain, 0)

        @pl.when(start < chunks)
        def _():
            for strip in strips:
                send_strip(strip).wait_send()

    total = add_rows(pair, part, rows_in, row_send, row_recv, all_in, drain_all)
    gap_out[...] = jnp.broadcast_to(total * inverse, gap_out.shape)


def whole_store_kernel(*refs):
    sources, gap, targets, sem, one = refs[:3], refs[3], refs[4:8], refs[8], refs[9]
    one[...] = gap[:, :1]
    pairs = zip((one, *sources), (targets[3], *targets[:3]))
    copies = [pltpu.make_async_copy(a, b, sem.at[i]) for i, (a, b) in enumerate(pairs)]
    for copy in copies:
        copy.start()
    for copy in copies:
        copy.wait()


def early_store_kernel(bit, chunks, mine, shared, peer, part, mine_hbm, shared_hbm, peer_hbm, part_out, sem, shared_sem):
    stop = by_place(bit, EARLY, chunks)
    cols = shared.shape[1]

    def copies(k):
        here = area(k, cols)
        return [
            pltpu.make_async_copy(a.at[here], b.at[here], sem.at[i, k])
            for i, (a, b) in enumerate(((mine, mine_hbm), (peer, peer_hbm)))
        ]

    whole = pltpu.make_async_copy(shared, shared_hbm, shared_sem)
    whole.start()

    def start(k, carry):
        for copy in copies(k):
            copy.start()
        return carry

    def wait(k, carry):
        for copy in copies(k):
            copy.wait()
        return carry

    lax.fori_loop(0, stop, start, 0)
    part_out[...] = part[...]
    whole.wait()
    lax.fori_loop(0, stop, wait, 0)


def late_store_kernel(
    bit, chunks, mine, peer, mine_tail, peer_tail, gap, mine_old, peer_old, mine_hbm, peer_hbm, gap_hbm, sem, gap_sem, one
):
    first, start = by_place(bit, EARLY, chunks), cut(bit, chunks)
    cols = mine_hbm.shape[1]

    def copies(k, tail):
        here = area(k, cols)
        pairs = ((mine_tail, mine_hbm), (peer_tail, peer_hbm)) if tail else ((mine, mine_hbm), (peer, peer_hbm))
        return [
            pltpu.make_async_copy(a.at[k - start] if tail else a.at[here], b.at[here], sem.at[i, k])
            for i, (a, b) in enumerate(pairs)
        ]

    one[...] = gap[:, :1]
    small = pltpu.make_async_copy(one, gap_hbm, gap_sem)
    small.start()

    def begin(tail, k, carry):
        for copy in copies(k, tail):
            copy.start()
        return carry

    def wait(tail, k, carry):
        for copy in copies(k, tail):
            copy.wait()
        return carry

    lax.fori_loop(first, start, partial(begin, False), 0)
    lax.fori_loop(start, chunks, partial(begin, True), 0)
    small.wait()
    lax.fori_loop(first, start, partial(wait, False), 0)
    lax.fori_loop(start, chunks, partial(wait, True), 0)


def shape(*dims):
    return pltpu.HBM(dims, jnp.float32)


def params_of(limit, collective_id=None):
    if collective_id is None:
        return pltpu.CompilerParams(vmem_limit_bytes=limit)
    return pltpu.CompilerParams(
        collective_id=collective_id, has_side_effects=True, vmem_limit_bytes=limit
    )


def cost(array, passes):
    return pl.CostEstimate(flops=passes * array.size, bytes_accessed=passes * array.size, transcendentals=0)


def row_scratch(n):
    return [
        pltpu.SemaphoreType.REGULAR,
        pltpu.SemaphoreType.REGULAR,
        pltpu.VMEM((1, STRIP), jnp.float32),
        pltpu.VMEM((n, 1, STRIP), jnp.float32),
        pltpu.SemaphoreType.DMA,
        pltpu.SemaphoreType.DMA,
    ]


def open_round(bit, last, params, public, peer_public):
    rows, cols = params.shape
    chunks = rows // BLOCK * (cols // WIDE)
    n = lax.axis_size("node")
    lead = chunks if last else min(2, chunks)
    full = pltpu.VMEM(params.shape, jnp.float32)
    levels = (chunks, BLOCK, WIDE)
    scales = (chunks // 2, 2, WIDE)
    sems = [pltpu.SemaphoreType.DMA((2, chunks)), pltpu.SemaphoreType.DMA((2, WIDE // STRIP))]
    sems += [pltpu.SemaphoreType.DMA((chunks,))]
    sems += [pltpu.SemaphoreType.DMA((2, chunks))] * 2
    out = [full, full, full]
    scratch = [pltpu.VMEM(levels, jnp.bfloat16), pltpu.VMEM(scales, jnp.bfloat16), pltpu.VMEM(scales, jnp.bfloat16)]
    if last:
        out += [pltpu.VMEM((1, STRIP), jnp.float32)]
        scratch = [pltpu.VMEM(levels, jnp.bfloat16)] + scratch + sems + row_scratch(n)
    else:
        out += [pltpu.VMEM(levels, jnp.bfloat16), pltpu.VMEM(scales, jnp.bfloat16), pltpu.VMEM((1, STRIP), jnp.float32)]
        scratch = scratch + sems
    return pl.pallas_call(
        partial(first_kernel, bit, lead, last, 1.0 / (n * rows * cols)),
        in_specs=[ANY] * 3,
        out_specs=[VMEM] * len(out),
        out_shape=out,
        scratch_shapes=scratch,
        cost_estimate=cost(params, 30),
        compiler_params=params_of(24 << 20, 2 * bit + 1),
    )(params, public, peer_public)


def close_round(bit, chunks, *arrays):
    rows, cols = arrays[0].shape
    n = lax.axis_size("node")
    rest = chunks - min(chunks * f // 16 for row in FIRST for f in row)
    tail = pltpu.VMEM((rest, BLOCK, WIDE), jnp.float32)
    return pl.pallas_call(
        partial(last_kernel, bit, 1.0 / (n * rows * cols)),
        in_specs=[VMEM] * 6,
        out_specs=[VMEM] * 3,
        out_shape=[tail, tail, pltpu.VMEM((1, STRIP), jnp.float32)],
        scratch_shapes=[
            pltpu.VMEM((rest, BLOCK, WIDE), jnp.bfloat16),
            pltpu.SemaphoreType.DMA((2, chunks)),
            pltpu.SemaphoreType.DMA((2, chunks)),
        ]
        + row_scratch(n),
        cost_estimate=cost(arrays[0], 10),
        compiler_params=params_of(8 << 20, 2 * bit + 2),
    )(*arrays)


def store_all(*arrays):
    return pl.pallas_call(
        whole_store_kernel,
        in_specs=[VMEM] * 4,
        out_specs=[HBM] * 4,
        out_shape=[shape(*a.shape) for a in arrays[:3]] + [shape(1, 1)],
        scratch_shapes=[pltpu.SemaphoreType.DMA((4,)), pltpu.VMEM((1, 1), jnp.float32)],
        compiler_params=params_of(1 << 20),
    )(*arrays)


def store_early(bit, chunks, mine, shared, peer, part):
    return pl.pallas_call(
        partial(early_store_kernel, bit, chunks),
        in_specs=[VMEM] * 4,
        out_specs=[HBM] * 3 + [VMEM],
        out_shape=[shape(*mine.shape)] * 3 + [pltpu.VMEM(part.shape, jnp.float32)],
        scratch_shapes=[pltpu.SemaphoreType.DMA((2, chunks)), pltpu.SemaphoreType.DMA],
        compiler_params=params_of(1 << 20),
    )(mine, shared, peer, part)


def store_late(bit, chunks, mine, peer, mine_tail, peer_tail, gap, mine_hbm, peer_hbm):
    return pl.pallas_call(
        partial(late_store_kernel, bit, chunks),
        in_specs=[VMEM] * 5 + [HBM] * 2,
        out_specs=[HBM] * 3,
        out_shape=[shape(*mine_hbm.shape)] * 2 + [shape(1, 1)],
        input_output_aliases={5: 0, 6: 1},
        scratch_shapes=[
            pltpu.SemaphoreType.DMA((2, chunks)),
            pltpu.SemaphoreType.DMA,
            pltpu.VMEM((1, 1), jnp.float32),
        ],
        compiler_params=params_of(1 << 20),
    )(mine, peer, mine_tail, peer_tail, gap, mine_hbm, peer_hbm)


def round_of(bit, params, public, peer_public):
    if bit == 0:
        return store_all(*open_round(bit, True, params, public, peer_public))
    mine, shared, peer, coded, scale, part = open_round(bit, False, params, public, peer_public)
    chunks = coded.shape[0]
    params_new, public_new, peer_new, part = store_early(bit, chunks, mine, shared, peer, part)
    *tails, gap = close_round(bit, chunks, mine, shared, peer, coded, scale, part)
    params_new, peer_new, gap = store_late(bit, chunks, mine, peer, *tails, gap, params_new, peer_new)
    return params_new, public_new, peer_new, gap


def shards(params, public, peer_public, round_index):
    n = lax.axis_size("node")
    bit_count = n.bit_length() - 1
    chosen_bit = lax.rem(round_index[0], jnp.int32(bit_count))
    branches = [partial(round_of, bit) for bit in range(bit_count)]
    params_new, public_new, peer_new, gap = lax.switch(
        chosen_bit, branches, params, public, peer_public
    )
    return (params_new, public_new, peer_new, gap[0, 0])


def solution(mesh):
    in_specs = (P("node", None), P("node", None), P("node", None), P())
    out_specs = (P("node", None), P("node", None), P("node", None), P())
    return jax.shard_map(shards, mesh=mesh, in_specs=in_specs, out_specs=out_specs, check_vma=False)
```

```python
from functools import partial

import jax
import jax.numpy as jnp
from jax import lax
from jax.experimental import pallas as pl
from jax.experimental.pallas import tpu as pltpu
from jax.sharding import PartitionSpec as P

BLOCK = 128
MIX = 0.4
WIDE = 512
STRIP = 128
SUBLANES = 8
FIRST = ((8, 16), (16, 10))
EARLY = ((8, 10), (16, 10))
MESH = pl.DeviceIdType.MESH
ANY = pl.BlockSpec(memory_space=pl.ANY)
VMEM = pl.BlockSpec(memory_space=pltpu.VMEM)
HBM = pl.BlockSpec(memory_space=pltpu.HBM)


def place(k, col_count):
    across = col_count // WIDE
    rows = pl.ds(pl.multiple_of(k // across * BLOCK, BLOCK), BLOCK)
    return rows, pl.multiple_of(k % across * WIDE, WIDE)


def area(k, col_count):
    rows, first = place(k, col_count)
    return rows, pl.ds(first, WIDE)


def by_place(bit, table, chunks):
    me, mask = lax.axis_index("node"), 1 << bit
    rows = [[chunks * sixteenths // 16 for sixteenths in row] for row in table]
    usual, other = (first + (second - first) * (me % 2) for first, second in rows)
    if 2 * mask == lax.axis_size("node"):
        return other
    low = me - mask * (me // mask % 2)
    return other + (usual - other) * jnp.minimum(low // 2, 1)


def cut(bit, chunks):
    return by_place(bit, FIRST, chunks)


class Pair:
    def __init__(self, bit, send_sem, recv_sem):
        self.me = lax.axis_index("node")
        self.mask = 1 << bit
        upper = self.me // self.mask % 2
        self.other = self.me + self.mask - 2 * self.mask * upper
        self.mixed = min(bit, 1)
        self.second = (upper + self.mixed * self.me) % 2
        self.sibling = self.me + 1 - 2 * (self.me % 2)
        self.send_sem, self.recv_sem = send_sem, recv_sem

    def tell(self, sem):
        pl.semaphore_signal(sem, inc=1, device_id=(self.other,), device_id_type=MESH)

    def copy(self, source, target, part, k):
        return pltpu.make_async_remote_copy(
            src_ref=source,
            dst_ref=target,
            send_sem=self.send_sem.at[part, k],
            recv_sem=self.recv_sem.at[part, k],
            device_id=(self.other,),
            device_id_type=MESH,
        )


def merge(k, slot, total, got_coded, got_scale, mine, shared, peer, mine_new, peer_new, spot, before=None):
    rows, first = place(k, shared.shape[1])
    for strip in range(0, WIDE, STRIP):
        if before is not None:
            before(strip)
        columns = pl.ds(pl.multiple_of(first + strip, STRIP), STRIP)
        both = got_scale[k // 2, :, strip : strip + STRIP].astype(jnp.float32) * (1.0 / 127.0)
        factor = jnp.where(k % 2 == 0, both[:1], both[1:])
        level = got_coded[slot, :, strip : strip + STRIP].astype(jnp.float32)
        theirs = peer[rows, columns] + level * factor
        public_new = shared[rows, columns]
        params_new = mine[rows, columns] + MIX * (theirs - public_new)
        target = spot(rows, columns, strip)
        peer_new[target] = theirs
        mine_new[target] = params_new
        distance = params_new - public_new
        total = total + jnp.sum((distance * distance).reshape(-1, SUBLANES, STRIP), axis=0)
    return total


def greet_pairs(pair, n, barrier):
    half, mask = n // 2, pair.mask
    mine = pair.me // (2 * mask) * mask + pair.me % mask

    def greet(k, carry):
        t = lax.rem(mine + k, half)
        low = t // mask * (2 * mask) + t % mask
        target = low + pair.mixed * mask * (low % 2)
        pl.semaphore_signal(barrier, inc=1, device_id=(target,), device_id_type=MESH)
        return carry

    lax.fori_loop(1, half, greet, 0)


def hear_pairs(pair, n, barrier, all_in):
    @pl.when(pair.second == 0)
    def _():
        pl.semaphore_wait(barrier, n - 2)
        pl.semaphore_signal(all_in, inc=1, device_id=(pair.sibling,), device_id_type=MESH)


def add_rows(pair, part, rows_in, row_send, row_recv, all_in, drain):
    n = rows_in.shape[0]

    @pl.when(pair.second == 1)
    def _():
        pl.semaphore_wait(all_in, 1)

    def row_copy(source, place, target):
        return pltpu.make_async_remote_copy(
            src_ref=source,
            dst_ref=place,
            send_sem=row_send,
            recv_sem=row_recv,
            device_id=(target,),
            device_id_type=MESH,
        )

    def send_row(k, carry):
        row_copy(part, rows_in.at[pair.me], lax.rem(pair.me + k, n)).start()
        return carry

    lax.fori_loop(1, n, send_row, 0)
    rows_in[pair.me] = part[...]
    drain()
    rest = rows_in.at[pl.ds(1, n - 1)]
    row_copy(rest, rest, pair.other).wait()
    return jnp.sum(jnp.sum(rows_in[...], axis=0), axis=1, keepdims=True)


def first_kernel(bit, lead, last, inverse, params_hbm, public_hbm, peer_hbm, *refs):
    mine, shared, peer = refs[:3]
    if last:
        gap_out, coded, got_coded, got_scale = refs[3:7]
        scale, load_sem, strip_sem, peer_sem, send_sem, recv_sem = refs[7:13]
        ready, all_in, part, rows_in, row_send, row_recv = refs[13:]
    else:
        coded, scale_out, part, got_coded, got_scale = refs[3:8]
        scale, load_sem, strip_sem, peer_sem, send_sem, recv_sem = refs[8:]
    chunks = coded.shape[0]
    cols = shared.shape[1]
    stop = chunks if last else cut(bit, chunks)
    pair = Pair(bit, send_sem, recv_sem)
    barrier = pltpu.get_barrier_semaphore()

    if last:

        @pl.when(pair.second == 0)
        def _():
            pair.tell(barrier)

        greet_pairs(pair, rows_in.shape[0], barrier)
    else:
        pair.tell(barrier)

    def load(k, source, target, sem):
        here = area(k, cols)
        return pltpu.make_async_copy(source.at[here], target.at[here], sem)

    def send_coded(k):
        return pair.copy(coded.at[k], got_coded.at[k], 0, k)

    def send_scale(i):
        return pair.copy(scale.at[i], got_scale.at[i], 1, i)

    def send_rest():
        rest = pl.ds(lead // 2, (chunks - lead) // 2)
        return pair.copy(scale.at[rest], got_scale.at[rest], 1, lead // 2)

    def load_strip(i, strip):
        here = (pl.ds(0, BLOCK), pl.ds(strip, STRIP))
        source, target = ((params_hbm, mine), (public_hbm, shared))[i]
        return pltpu.make_async_copy(source.at[here], target.at[here], strip_sem.at[i, strip // STRIP])

    def send_strip(strip):
        here = (0, slice(None), pl.ds(strip, STRIP))
        return pair.copy(coded.at[here], got_coded.at[here], 0, 0)

    for strip in range(0, WIDE, STRIP):
        for i in range(2):
            load_strip(i, strip).start()

    def begin(k, carry):
        load(k, params_hbm, mine, load_sem.at[0, k]).start()
        load(k, public_hbm, shared, load_sem.at[1, k]).start()
        return carry

    lax.fori_loop(1, chunks, begin, 0)

    if last:

        @pl.when(pair.second == 1)
        def _():
            pl.semaphore_wait(barrier, 1)
            pair.tell(ready)

    def met():
        if last:

            @pl.when(pair.second == 0)
            def _():
                pl.semaphore_wait(ready, 1)
        else:
            pl.semaphore_wait(barrier, 1)

    def encode(k, opening):
        rows, first = place(k, cols)
        if not opening:
            load(k, params_hbm, mine, load_sem.at[0, k]).wait()
            load(k, public_hbm, shared, load_sem.at[1, k]).wait()
        scales = []
        for strip in range(0, WIDE, STRIP):
            if opening:
                for i in range(2):
                    load_strip(i, strip).wait()
            columns = pl.ds(pl.multiple_of(first + strip, STRIP), STRIP)
            difference = mine[rows, columns] - shared[rows, columns]
            peak = jnp.max(jnp.abs(difference), axis=0, keepdims=True) + 1e-06
            wide = peak.astype(jnp.bfloat16).astype(jnp.float32)
            level = jnp.floor(difference * (127.0 / wide) + 0.5)
            coded[k, :, strip : strip + STRIP] = level.astype(jnp.bfloat16)
            if opening:
                if strip == 0:
                    met()
                send_strip(strip).start()
            shared[rows, columns] = shared[rows, columns] + level * (wide * (1.0 / 127.0))
            scales.append(wide)
        return scales

    def encode_two(i, opening):
        k = 2 * i
        even = encode(k, opening)
        if not opening:

            @pl.when(k < lead)
            def _():
                send_coded(k).start()

        odd = encode(k + 1, False)
        first_row = lax.broadcasted_iota(jnp.int32, (2, STRIP), 0) == 0
        for strip, a, b in zip(range(0, WIDE, STRIP), even, odd):
            scale[i, :, strip : strip + STRIP] = jnp.where(first_row, a, b).astype(jnp.bfloat16)

        @pl.when(k < lead)
        def _():
            send_scale(i).start()
            send_coded(k + 1).start()

        for h in range(2):
            load(k + h, peer_hbm, peer, peer_sem.at[k + h]).start()

    def encode_later(i, carry):
        encode_two(i, False)
        return carry

    encode_two(0, True)
    lax.fori_loop(1, chunks // 2, encode_later, 0)

    if lead < chunks:
        send_rest().start()

        def send_more(k, carry):
            send_coded(k).start()
            return carry

        lax.fori_loop(lead, stop, send_more, 0)

    def combine(k, total):
        load(k, peer_hbm, peer, peer_sem.at[k]).wait()
        if last:

            @pl.when(k == chunks - 1)
            def _():
                hear_pairs(pair, rows_in.shape[0], barrier, all_in)

        @pl.when((k < lead) & (k % 2 == 0))
        def _():
            send_scale(k // 2).wait()

        if lead < chunks:

            @pl.when(k == lead)
            def _():
                send_rest().wait()

        send_coded(k).wait()
        return merge(
            k, k, total, got_coded, got_scale, mine, shared, peer, mine, peer,
            lambda rows, columns, strip: (rows, columns),
        )

    def land(k, carry):
        load(k, peer_hbm, peer, peer_sem.at[k]).wait()
        return carry

    lax.fori_loop(stop, chunks, land, 0)
    total = lax.fori_loop(0, stop, combine, jnp.zeros((SUBLANES, STRIP), jnp.float32))
    part[...] = jnp.sum(total, axis=0, keepdims=True) if last else total

    if last:
        total = add_rows(pair, part, rows_in, row_send, row_recv, all_in, lambda: None)
        gap_out[...] = jnp.broadcast_to(total * inverse, gap_out.shape)
    else:
        scale_out[...] = got_scale[...]


def last_kernel(bit, inverse, mine, shared, peer, coded, got_scale, part_in, *refs):
    mine_new, peer_new, gap_out, got_coded, send_sem, recv_sem, sums = refs[:7]
    ready, all_in, part, rows_in, row_send, row_recv = refs[7:]
    chunks = coded.shape[0]
    start = cut(bit, chunks)
    pair = Pair(bit, send_sem, recv_sem)
    n = rows_in.shape[0]
    barrier = pltpu.get_barrier_semaphore()

    @pl.when(pair.second == 0)
    def _():
        pair.tell(barrier)

    greet_pairs(pair, n, barrier)

    @pl.when(pair.second == 1)
    def _():
        pl.semaphore_wait(barrier, 1)
        pair.tell(ready)

    @pl.when(pair.second == 0)
    def _():
        pl.semaphore_wait(ready, 1)

    def send_coded(k):
        return pair.copy(coded.at[k], got_coded.at[k - start], 0, k)

    end = chunks - 1

    def send_strip(strip):
        columns = pl.ds(strip, STRIP)
        source, target = coded.at[end, :, columns], got_coded.at[end - start, :, columns]
        return pair.copy(source, target, 1, strip // STRIP)

    strips = range(0, WIDE, STRIP)

    def send(k, carry):
        send_coded(k).start()
        return carry

    lax.fori_loop(start, end, send, 0)

    @pl.when(start < chunks)
    def _():
        for strip in strips:
            send_strip(strip).start()

    def combine(k, total, before=None):
        slot = k - start
        return merge(
            k, slot, total, got_coded, got_scale, mine, shared, peer, mine_new, peer_new,
            lambda rows, columns, strip: (slot, slice(None), slice(strip, strip + STRIP)), before
        )

    def take(k, total):
        send_coded(k).wait_recv()
        return combine(k, total)

    sums[...] = lax.fori_loop(start, end, take, part_in[...])
    hear_pairs(pair, n, barrier, all_in)

    @pl.when(start < chunks)
    def _():
        sums[...] = combine(end, sums[...], lambda strip: send_strip(strip).wait_recv())

    part[...] = jnp.sum(sums[...], axis=0, keepdims=True)

    def drain(k, carry):
        send_coded(k).wait_send()
        return carry

    def drain_all():
        lax.fori_loop(start, end, drain, 0)

        @pl.when(start < chunks)
        def _():
            for strip in strips:
                send_strip(strip).wait_send()

    total = add_rows(pair, part, rows_in, row_send, row_recv, all_in, drain_all)
    gap_out[...] = jnp.broadcast_to(total * inverse, gap_out.shape)


def whole_store_kernel(*refs):
    sources, gap, targets, sem, one = refs[:3], refs[3], refs[4:8], refs[8], refs[9]
    one[...] = gap[:, :1]
    pairs = zip((one, *sources), (targets[3], *targets[:3]))
    copies = [pltpu.make_async_copy(a, b, sem.at[i]) for i, (a, b) in enumerate(pairs)]
    for copy in copies:
        copy.start()
    for copy in copies:
        copy.wait()


def early_store_kernel(bit, chunks, mine, shared, peer, part, mine_hbm, shared_hbm, peer_hbm, part_out, sem, shared_sem):
    stop = by_place(bit, EARLY, chunks)
    cols = shared.shape[1]

    def copies(k):
        here = area(k, cols)
        return [
            pltpu.make_async_copy(a.at[here], b.at[here], sem.at[i, k])
            for i, (a, b) in enumerate(((mine, mine_hbm), (peer, peer_hbm)))
        ]

    whole = pltpu.make_async_copy(shared, shared_hbm, shared_sem)
    whole.start()

    def start(k, carry):
        for copy in copies(k):
            copy.start()
        return carry

    def wait(k, carry):
        for copy in copies(k):
            copy.wait()
        return carry

    lax.fori_loop(0, stop, start, 0)
    part_out[...] = part[...]
    whole.wait()
    lax.fori_loop(0, stop, wait, 0)


def late_store_kernel(
    bit, chunks, mine, peer, mine_tail, peer_tail, gap, mine_old, peer_old, mine_hbm, peer_hbm, gap_hbm, sem, gap_sem, one
):
    first, start = by_place(bit, EARLY, chunks), cut(bit, chunks)
    cols = mine_hbm.shape[1]

    def copies(k, tail):
        here = area(k, cols)
        pairs = ((mine_tail, mine_hbm), (peer_tail, peer_hbm)) if tail else ((mine, mine_hbm), (peer, peer_hbm))
        return [
            pltpu.make_async_copy(a.at[k - start] if tail else a.at[here], b.at[here], sem.at[i, k])
            for i, (a, b) in enumerate(pairs)
        ]

    one[...] = gap[:, :1]
    small = pltpu.make_async_copy(one, gap_hbm, gap_sem)
    small.start()

    def begin(tail, k, carry):
        for copy in copies(k, tail):
            copy.start()
        return carry

    def wait(tail, k, carry):
        for copy in copies(k, tail):
            copy.wait()
        return carry

    lax.fori_loop(first, start, partial(begin, False), 0)
    lax.fori_loop(start, chunks, partial(begin, True), 0)
    small.wait()
    lax.fori_loop(first, start, partial(wait, False), 0)
    lax.fori_loop(start, chunks, partial(wait, True), 0)


def shape(*dims):
    return pltpu.HBM(dims, jnp.float32)


def params_of(limit, collective_id=None):
    if collective_id is None:
        return pltpu.CompilerParams(vmem_limit_bytes=limit)
    return pltpu.CompilerParams(
        collective_id=collective_id, has_side_effects=True, vmem_limit_bytes=limit
    )


def cost(array, passes):
    return pl.CostEstimate(flops=passes * array.size, bytes_accessed=passes * array.size, transcendentals=0)


def row_scratch(n):
    return [
        pltpu.SemaphoreType.REGULAR,
        pltpu.SemaphoreType.REGULAR,
        pltpu.VMEM((1, STRIP), jnp.float32),
        pltpu.VMEM((n, 1, STRIP), jnp.float32),
        pltpu.SemaphoreType.DMA,
        pltpu.SemaphoreType.DMA,
    ]


def open_round(bit, last, params, public, peer_public):
    rows, cols = params.shape
    chunks = rows // BLOCK * (cols // WIDE)
    n = lax.axis_size("node")
    lead = chunks if last else min(2, chunks)
    full = pltpu.VMEM(params.shape, jnp.float32)
    levels = (chunks, BLOCK, WIDE)
    scales = (chunks // 2, 2, WIDE)
    sems = [pltpu.SemaphoreType.DMA((2, chunks)), pltpu.SemaphoreType.DMA((2, WIDE // STRIP))]
    sems += [pltpu.SemaphoreType.DMA((chunks,))]
    sems += [pltpu.SemaphoreType.DMA((2, chunks))] * 2
    out = [full, full, full]
    scratch = [pltpu.VMEM(levels, jnp.bfloat16), pltpu.VMEM(scales, jnp.bfloat16), pltpu.VMEM(scales, jnp.bfloat16)]
    if last:
        out += [pltpu.VMEM((1, STRIP), jnp.float32)]
        scratch = [pltpu.VMEM(levels, jnp.bfloat16)] + scratch + sems + row_scratch(n)
    else:
        out += [pltpu.VMEM(levels, jnp.bfloat16), pltpu.VMEM(scales, jnp.bfloat16), pltpu.VMEM((SUBLANES, STRIP), jnp.float32)]
        scratch = scratch + sems
    return pl.pallas_call(
        partial(first_kernel, bit, lead, last, 1.0 / (n * rows * cols)),
        in_specs=[ANY] * 3,
        out_specs=[VMEM] * len(out),
        out_shape=out,
        scratch_shapes=scratch,
        cost_estimate=cost(params, 30),
        compiler_params=params_of(24 << 20, 2 * bit + 1),
    )(params, public, peer_public)


def close_round(bit, chunks, *arrays):
    rows, cols = arrays[0].shape
    n = lax.axis_size("node")
    rest = chunks - min(chunks * f // 16 for row in FIRST for f in row)
    tail = pltpu.VMEM((rest, BLOCK, WIDE), jnp.float32)
    return pl.pallas_call(
        partial(last_kernel, bit, 1.0 / (n * rows * cols)),
        in_specs=[VMEM] * 6,
        out_specs=[VMEM] * 3,
        out_shape=[tail, tail, pltpu.VMEM((1, STRIP), jnp.float32)],
        scratch_shapes=[
            pltpu.VMEM((rest, BLOCK, WIDE), jnp.bfloat16),
            pltpu.SemaphoreType.DMA((2, chunks)),
            pltpu.SemaphoreType.DMA((2, chunks)),
            pltpu.VMEM((SUBLANES, STRIP), jnp.float32),
        ]
        + row_scratch(n),
        cost_estimate=cost(arrays[0], 10),
        compiler_params=params_of(8 << 20, 2 * bit + 2),
    )(*arrays)


def store_all(*arrays):
    return pl.pallas_call(
        whole_store_kernel,
        in_specs=[VMEM] * 4,
        out_specs=[HBM] * 4,
        out_shape=[shape(*a.shape) for a in arrays[:3]] + [shape(1, 1)],
        scratch_shapes=[pltpu.SemaphoreType.DMA((4,)), pltpu.VMEM((1, 1), jnp.float32)],
        compiler_params=params_of(1 << 20),
    )(*arrays)


def store_early(bit, chunks, mine, shared, peer, part):
    return pl.pallas_call(
        partial(early_store_kernel, bit, chunks),
        in_specs=[VMEM] * 4,
        out_specs=[HBM] * 3 + [VMEM],
        out_shape=[shape(*mine.shape)] * 3 + [pltpu.VMEM(part.shape, jnp.float32)],
        scratch_shapes=[pltpu.SemaphoreType.DMA((2, chunks)), pltpu.SemaphoreType.DMA],
        compiler_params=params_of(1 << 20),
    )(mine, shared, peer, part)


def store_late(bit, chunks, mine, peer, mine_tail, peer_tail, gap, mine_hbm, peer_hbm):
    return pl.pallas_call(
        partial(late_store_kernel, bit, chunks),
        in_specs=[VMEM] * 5 + [HBM] * 2,
        out_specs=[HBM] * 3,
        out_shape=[shape(*mine_hbm.shape)] * 2 + [shape(1, 1)],
        input_output_aliases={5: 0, 6: 1},
        scratch_shapes=[
            pltpu.SemaphoreType.DMA((2, chunks)),
            pltpu.SemaphoreType.DMA,
            pltpu.VMEM((1, 1), jnp.float32),
        ],
        compiler_params=params_of(1 << 20),
    )(mine, peer, mine_tail, peer_tail, gap, mine_hbm, peer_hbm)


def round_of(bit, params, public, peer_public):
    if bit == 0:
        return store_all(*open_round(bit, True, params, public, peer_public))
    mine, shared, peer, coded, scale, part = open_round(bit, False, params, public, peer_public)
    chunks = coded.shape[0]
    params_new, public_new, peer_new, part = store_early(bit, chunks, mine, shared, peer, part)
    *tails, gap = close_round(bit, chunks, mine, shared, peer, coded, scale, part)
    params_new, peer_new, gap = store_late(bit, chunks, mine, peer, *tails, gap, params_new, peer_new)
    return params_new, public_new, peer_new, gap


def shards(params, public, peer_public, round_index):
    n = lax.axis_size("node")
    bit_count = n.bit_length() - 1
    chosen_bit = lax.rem(round_index[0], jnp.int32(bit_count))
    branches = [partial(round_of, bit) for bit in range(bit_count)]
    params_new, public_new, peer_new, gap = lax.switch(
        chosen_bit, branches, params, public, peer_public
    )
    return (params_new, public_new, peer_new, gap[0, 0])


def solution(mesh):
    in_specs = (P("node", None), P("node", None), P("node", None), P())
    out_specs = (P("node", None), P("node", None), P("node", None), P())
    return jax.shard_map(shards, mesh=mesh, in_specs=in_specs, out_specs=out_specs, check_vma=False)
```

```python
from functools import partial

import jax
import jax.numpy as jnp
from jax import lax
from jax.experimental import pallas as pl
from jax.experimental.pallas import tpu as pltpu
from jax.sharding import PartitionSpec as P

BLOCK = 128
MIX = 0.4
WIDE = 512
STRIP = 128
SUBLANES = 8
FIRST = ((8, 16), (16, 10))
EARLY = ((8, 10), (16, 10))
MESH = pl.DeviceIdType.MESH
ANY = pl.BlockSpec(memory_space=pl.ANY)
VMEM = pl.BlockSpec(memory_space=pltpu.VMEM)
HBM = pl.BlockSpec(memory_space=pltpu.HBM)


def place(k, col_count):
    across = col_count // WIDE
    rows = pl.ds(pl.multiple_of(k // across * BLOCK, BLOCK), BLOCK)
    return rows, pl.multiple_of(k % across * WIDE, WIDE)


def area(k, col_count):
    rows, first = place(k, col_count)
    return rows, pl.ds(first, WIDE)


def by_place(bit, table, chunks):
    me, mask = lax.axis_index("node"), 1 << bit
    rows = [[chunks * sixteenths // 16 for sixteenths in row] for row in table]
    usual, other = (first + (second - first) * (me % 2) for first, second in rows)
    if 2 * mask == lax.axis_size("node"):
        return other
    low = me - mask * (me // mask % 2)
    return other + (usual - other) * jnp.minimum(low // 2, 1)


def cut(bit, chunks):
    return by_place(bit, FIRST, chunks)


class Pair:
    def __init__(self, bit, send_sem, recv_sem):
        self.me = lax.axis_index("node")
        self.mask = 1 << bit
        upper = self.me // self.mask % 2
        self.other = self.me + self.mask - 2 * self.mask * upper
        self.mixed = min(bit, 1)
        self.second = (upper + self.mixed * self.me) % 2
        self.sibling = self.me + 1 - 2 * (self.me % 2)
        self.send_sem, self.recv_sem = send_sem, recv_sem

    def tell(self, sem):
        pl.semaphore_signal(sem, inc=1, device_id=(self.other,), device_id_type=MESH)

    def copy(self, source, target, part, k):
        return pltpu.make_async_remote_copy(
            src_ref=source,
            dst_ref=target,
            send_sem=self.send_sem.at[part, k],
            recv_sem=self.recv_sem.at[part, k],
            device_id=(self.other,),
            device_id_type=MESH,
        )


def merge(k, slot, total, got_coded, got_scale, mine, shared, peer, mine_new, peer_new, spot, before=None):
    rows, first = place(k, shared.shape[1])
    for strip in range(0, WIDE, STRIP):
        if before is not None:
            before(strip)
        columns = pl.ds(pl.multiple_of(first + strip, STRIP), STRIP)
        both = got_scale[k // 2, :, strip : strip + STRIP].astype(jnp.float32) * (1.0 / 127.0)
        factor = jnp.where(k % 2 == 0, both[:1], both[1:])
        level = got_coded[slot, :, strip : strip + STRIP].astype(jnp.float32)
        theirs = peer[rows, columns] + level * factor
        public_new = shared[rows, columns]
        params_new = mine[rows, columns] + MIX * (theirs - public_new)
        target = spot(rows, columns, strip)
        peer_new[target] = theirs
        mine_new[target] = params_new
        distance = params_new - public_new
        total = total + jnp.sum((distance * distance).reshape(-1, SUBLANES, STRIP), axis=0)
    return total


def greet_pairs(pair, n, barrier):
    half, mask = n // 2, pair.mask
    mine = pair.me // (2 * mask) * mask + pair.me % mask

    def greet(k, carry):
        t = lax.rem(mine + k, half)
        low = t // mask * (2 * mask) + t % mask
        target = low + pair.mixed * mask * (low % 2)
        pl.semaphore_signal(barrier, inc=1, device_id=(target,), device_id_type=MESH)
        return carry

    lax.fori_loop(1, half, greet, 0)


def hear_pairs(pair, n, barrier, all_in):
    @pl.when(pair.second == 0)
    def _():
        pl.semaphore_wait(barrier, n - 2)
        pl.semaphore_signal(all_in, inc=1, device_id=(pair.sibling,), device_id_type=MESH)


def add_rows(pair, part, rows_in, row_send, row_recv, all_in, drain):
    n = rows_in.shape[0]

    @pl.when(pair.second == 1)
    def _():
        pl.semaphore_wait(all_in, 1)

    def row_copy(source, place, target):
        return pltpu.make_async_remote_copy(
            src_ref=source,
            dst_ref=place,
            send_sem=row_send,
            recv_sem=row_recv,
            device_id=(target,),
            device_id_type=MESH,
        )

    def send_row(k, carry):
        row_copy(part, rows_in.at[pair.me], lax.rem(pair.me + k, n)).start()
        return carry

    lax.fori_loop(1, n, send_row, 0)
    rows_in[pair.me] = part[...]
    drain()
    rest = rows_in.at[pl.ds(1, n - 1)]
    row_copy(rest, rest, pair.other).wait()
    return jnp.sum(jnp.sum(rows_in[...], axis=0), axis=1, keepdims=True)


def first_kernel(bit, lead, last, inverse, params_hbm, public_hbm, peer_hbm, *refs):
    mine, shared, peer = refs[:3]
    if last:
        gap_out, coded, got_coded, got_scale = refs[3:7]
        scale, load_sem, strip_sem, peer_sem, send_sem, recv_sem = refs[7:13]
        ready, all_in, part, rows_in, row_send, row_recv = refs[13:]
    else:
        coded, scale_out, part, got_coded, got_scale = refs[3:8]
        scale, load_sem, strip_sem, peer_sem, send_sem, recv_sem = refs[8:]
    chunks = coded.shape[0]
    cols = shared.shape[1]
    stop = chunks if last else cut(bit, chunks)
    pair = Pair(bit, send_sem, recv_sem)
    barrier = pltpu.get_barrier_semaphore()

    if last:

        @pl.when(pair.second == 0)
        def _():
            pair.tell(barrier)

        greet_pairs(pair, rows_in.shape[0], barrier)
    else:
        pair.tell(barrier)

    def load(k, source, target, sem):
        here = area(k, cols)
        return pltpu.make_async_copy(source.at[here], target.at[here], sem)

    def send_coded(k):
        return pair.copy(coded.at[k], got_coded.at[k], 0, k)

    def send_scale(i):
        return pair.copy(scale.at[i], got_scale.at[i], 1, i)

    def send_rest():
        rest = pl.ds(lead // 2, (chunks - lead) // 2)
        return pair.copy(scale.at[rest], got_scale.at[rest], 1, lead // 2)

    def load_strip(i, strip):
        here = (pl.ds(0, BLOCK), pl.ds(strip, STRIP))
        source, target = ((params_hbm, mine), (public_hbm, shared))[i]
        return pltpu.make_async_copy(source.at[here], target.at[here], strip_sem.at[i, strip // STRIP])

    def send_strip(strip):
        here = (0, slice(None), pl.ds(strip, STRIP))
        return pair.copy(coded.at[here], got_coded.at[here], 0, 0)

    for strip in range(0, WIDE, STRIP):
        for i in range(2):
            load_strip(i, strip).start()

    def begin(k, carry):
        load(k, params_hbm, mine, load_sem.at[0, k]).start()
        load(k, public_hbm, shared, load_sem.at[1, k]).start()
        return carry

    lax.fori_loop(1, chunks, begin, 0)

    if last:

        @pl.when(pair.second == 1)
        def _():
            pl.semaphore_wait(barrier, 1)
            pair.tell(ready)

    def met():
        if last:

            @pl.when(pair.second == 0)
            def _():
                pl.semaphore_wait(ready, 1)
        else:
            pl.semaphore_wait(barrier, 1)

    def encode(k, opening):
        rows, first = place(k, cols)
        if not opening:
            load(k, params_hbm, mine, load_sem.at[0, k]).wait()
            load(k, public_hbm, shared, load_sem.at[1, k]).wait()
        scales = []
        for strip in range(0, WIDE, STRIP):
            if opening:
                for i in range(2):
                    load_strip(i, strip).wait()
            columns = pl.ds(pl.multiple_of(first + strip, STRIP), STRIP)
            difference = mine[rows, columns] - shared[rows, columns]
            peak = jnp.max(jnp.abs(difference), axis=0, keepdims=True) + 1e-06
            wide = peak.astype(jnp.bfloat16).astype(jnp.float32)
            level = jnp.floor(difference / wide * 127.0 + 0.5)
            coded[k, :, strip : strip + STRIP] = level.astype(jnp.bfloat16)
            if opening:
                if strip == 0:
                    met()
                send_strip(strip).start()
            shared[rows, columns] = shared[rows, columns] + level * (wide * (1.0 / 127.0))
            scales.append(wide)
        return scales

    def encode_two(i, opening):
        k = 2 * i
        even = encode(k, opening)
        if not opening:

            @pl.when(k < lead)
            def _():
                send_coded(k).start()

        odd = encode(k + 1, False)
        first_row = lax.broadcasted_iota(jnp.int32, (2, STRIP), 0) == 0
        for strip, a, b in zip(range(0, WIDE, STRIP), even, odd):
            scale[i, :, strip : strip + STRIP] = jnp.where(first_row, a, b).astype(jnp.bfloat16)

        @pl.when(k < lead)
        def _():
            send_scale(i).start()
            send_coded(k + 1).start()

        for h in range(2):
            load(k + h, peer_hbm, peer, peer_sem.at[k + h]).start()

    def encode_later(i, carry):
        encode_two(i, False)
        return carry

    encode_two(0, True)
    lax.fori_loop(1, chunks // 2, encode_later, 0)

    if lead < chunks:
        send_rest().start()

        def send_more(k, carry):
            send_coded(k).start()
            return carry

        lax.fori_loop(lead, stop, send_more, 0)

    def combine(k, total):
        load(k, peer_hbm, peer, peer_sem.at[k]).wait()
        if last:

            @pl.when(k == chunks - 1)
            def _():
                hear_pairs(pair, rows_in.shape[0], barrier, all_in)

        @pl.when((k < lead) & (k % 2 == 0))
        def _():
            send_scale(k // 2).wait()

        if lead < chunks:

            @pl.when(k == lead)
            def _():
                send_rest().wait()

        send_coded(k).wait()
        return merge(
            k, k, total, got_coded, got_scale, mine, shared, peer, mine, peer,
            lambda rows, columns, strip: (rows, columns),
        )

    def land(k, carry):
        load(k, peer_hbm, peer, peer_sem.at[k]).wait()
        return carry

    lax.fori_loop(stop, chunks, land, 0)
    total = lax.fori_loop(0, stop, combine, jnp.zeros((SUBLANES, STRIP), jnp.float32))
    part[...] = jnp.sum(total, axis=0, keepdims=True) if last else total

    if last:
        total = add_rows(pair, part, rows_in, row_send, row_recv, all_in, lambda: None)
        gap_out[...] = jnp.broadcast_to(total * inverse, gap_out.shape)
    else:
        scale_out[...] = got_scale[...]


def last_kernel(bit, inverse, mine, shared, peer, coded, got_scale, part_in, *refs):
    mine_new, peer_new, gap_out, got_coded, send_sem, recv_sem, sums = refs[:7]
    ready, all_in, part, rows_in, row_send, row_recv = refs[7:]
    chunks = coded.shape[0]
    start = cut(bit, chunks)
    pair = Pair(bit, send_sem, recv_sem)
    n = rows_in.shape[0]
    barrier = pltpu.get_barrier_semaphore()

    @pl.when(pair.second == 0)
    def _():
        pair.tell(barrier)

    greet_pairs(pair, n, barrier)

    @pl.when(pair.second == 1)
    def _():
        pl.semaphore_wait(barrier, 1)
        pair.tell(ready)

    @pl.when(pair.second == 0)
    def _():
        pl.semaphore_wait(ready, 1)

    def send_coded(k):
        return pair.copy(coded.at[k], got_coded.at[k - start], 0, k)

    end = chunks - 1

    def send_strip(strip):
        columns = pl.ds(strip, STRIP)
        source, target = coded.at[end, :, columns], got_coded.at[end - start, :, columns]
        return pair.copy(source, target, 1, strip // STRIP)

    strips = range(0, WIDE, STRIP)

    def send(k, carry):
        send_coded(k).start()
        return carry

    lax.fori_loop(start, end, send, 0)

    @pl.when(start < chunks)
    def _():
        for strip in strips:
            send_strip(strip).start()

    def combine(k, total, before=None):
        slot = k - start
        return merge(
            k, slot, total, got_coded, got_scale, mine, shared, peer, mine_new, peer_new,
            lambda rows, columns, strip: (slot, slice(None), slice(strip, strip + STRIP)), before
        )

    def take(k, total):
        send_coded(k).wait_recv()
        return combine(k, total)

    sums[...] = lax.fori_loop(start, end, take, part_in[...])
    hear_pairs(pair, n, barrier, all_in)

    @pl.when(start < chunks)
    def _():
        sums[...] = combine(end, sums[...], lambda strip: send_strip(strip).wait_recv())

    part[...] = jnp.sum(sums[...], axis=0, keepdims=True)

    def drain(k, carry):
        send_coded(k).wait_send()
        return carry

    def drain_all():
        lax.fori_loop(start, end, drain, 0)

        @pl.when(start < chunks)
        def _():
            for strip in strips:
                send_strip(strip).wait_send()

    total = add_rows(pair, part, rows_in, row_send, row_recv, all_in, drain_all)
    gap_out[...] = jnp.broadcast_to(total * inverse, gap_out.shape)


def whole_store_kernel(*refs):
    sources, gap, targets, sem, one = refs[:3], refs[3], refs[4:8], refs[8], refs[9]
    one[...] = gap[:, :1]
    pairs = zip((one, *sources), (targets[3], *targets[:3]))
    copies = [pltpu.make_async_copy(a, b, sem.at[i]) for i, (a, b) in enumerate(pairs)]
    for copy in copies:
        copy.start()
    for copy in copies:
        copy.wait()


def early_store_kernel(bit, chunks, mine, shared, peer, part, mine_hbm, shared_hbm, peer_hbm, part_out, sem, shared_sem):
    stop = by_place(bit, EARLY, chunks)
    cols = shared.shape[1]

    def copies(k):
        here = area(k, cols)
        return [
            pltpu.make_async_copy(a.at[here], b.at[here], sem.at[i, k])
            for i, (a, b) in enumerate(((mine, mine_hbm), (peer, peer_hbm)))
        ]

    whole = pltpu.make_async_copy(shared, shared_hbm, shared_sem)
    whole.start()

    def start(k, carry):
        for copy in copies(k):
            copy.start()
        return carry

    def wait(k, carry):
        for copy in copies(k):
            copy.wait()
        return carry

    lax.fori_loop(0, stop, start, 0)
    part_out[...] = part[...]
    whole.wait()
    lax.fori_loop(0, stop, wait, 0)


def late_store_kernel(
    bit, chunks, mine, peer, mine_tail, peer_tail, gap, mine_old, peer_old, mine_hbm, peer_hbm, gap_hbm, sem, gap_sem, one
):
    first, start = by_place(bit, EARLY, chunks), cut(bit, chunks)
    cols = mine_hbm.shape[1]

    def copies(k, tail):
        here = area(k, cols)
        pairs = ((mine_tail, mine_hbm), (peer_tail, peer_hbm)) if tail else ((mine, mine_hbm), (peer, peer_hbm))
        return [
            pltpu.make_async_copy(a.at[k - start] if tail else a.at[here], b.at[here], sem.at[i, k])
            for i, (a, b) in enumerate(pairs)
        ]

    one[...] = gap[:, :1]
    small = pltpu.make_async_copy(one, gap_hbm, gap_sem)
    small.start()

    def begin(tail, k, carry):
        for copy in copies(k, tail):
            copy.start()
        return carry

    def wait(tail, k, carry):
        for copy in copies(k, tail):
            copy.wait()
        return carry

    lax.fori_loop(first, start, partial(begin, False), 0)
    lax.fori_loop(start, chunks, partial(begin, True), 0)
    small.wait()
    lax.fori_loop(first, start, partial(wait, False), 0)
    lax.fori_loop(start, chunks, partial(wait, True), 0)


def shape(*dims):
    return pltpu.HBM(dims, jnp.float32)


def params_of(limit, collective_id=None):
    if collective_id is None:
        return pltpu.CompilerParams(vmem_limit_bytes=limit)
    return pltpu.CompilerParams(
        collective_id=collective_id, has_side_effects=True, vmem_limit_bytes=limit
    )


def cost(array, passes):
    return pl.CostEstimate(flops=passes * array.size, bytes_accessed=passes * array.size, transcendentals=0)


def row_scratch(n):
    return [
        pltpu.SemaphoreType.REGULAR,
        pltpu.SemaphoreType.REGULAR,
        pltpu.VMEM((1, STRIP), jnp.float32),
        pltpu.VMEM((n, 1, STRIP), jnp.float32),
        pltpu.SemaphoreType.DMA,
        pltpu.SemaphoreType.DMA,
    ]


def open_round(bit, last, params, public, peer_public):
    rows, cols = params.shape
    chunks = rows // BLOCK * (cols // WIDE)
    n = lax.axis_size("node")
    lead = chunks if last else min(2, chunks)
    full = pltpu.VMEM(params.shape, jnp.float32)
    levels = (chunks, BLOCK, WIDE)
    scales = (chunks // 2, 2, WIDE)
    sems = [pltpu.SemaphoreType.DMA((2, chunks)), pltpu.SemaphoreType.DMA((2, WIDE // STRIP))]
    sems += [pltpu.SemaphoreType.DMA((chunks,))]
    sems += [pltpu.SemaphoreType.DMA((2, chunks))] * 2
    out = [full, full, full]
    scratch = [pltpu.VMEM(levels, jnp.bfloat16), pltpu.VMEM(scales, jnp.bfloat16), pltpu.VMEM(scales, jnp.bfloat16)]
    if last:
        out += [pltpu.VMEM((1, STRIP), jnp.float32)]
        scratch = [pltpu.VMEM(levels, jnp.bfloat16)] + scratch + sems + row_scratch(n)
    else:
        out += [pltpu.VMEM(levels, jnp.bfloat16), pltpu.VMEM(scales, jnp.bfloat16), pltpu.VMEM((SUBLANES, STRIP), jnp.float32)]
        scratch = scratch + sems
    return pl.pallas_call(
        partial(first_kernel, bit, lead, last, 1.0 / (n * rows * cols)),
        in_specs=[ANY] * 3,
        out_specs=[VMEM] * len(out),
        out_shape=out,
        scratch_shapes=scratch,
        cost_estimate=cost(params, 30),
        compiler_params=params_of(24 << 20, 2 * bit + 1),
    )(params, public, peer_public)


def close_round(bit, chunks, *arrays):
    rows, cols = arrays[0].shape
    n = lax.axis_size("node")
    rest = chunks - min(chunks * f // 16 for row in FIRST for f in row)
    tail = pltpu.VMEM((rest, BLOCK, WIDE), jnp.float32)
    return pl.pallas_call(
        partial(last_kernel, bit, 1.0 / (n * rows * cols)),
        in_specs=[VMEM] * 6,
        out_specs=[VMEM] * 3,
        out_shape=[tail, tail, pltpu.VMEM((1, STRIP), jnp.float32)],
        scratch_shapes=[
            pltpu.VMEM((rest, BLOCK, WIDE), jnp.bfloat16),
            pltpu.SemaphoreType.DMA((2, chunks)),
            pltpu.SemaphoreType.DMA((2, chunks)),
            pltpu.VMEM((SUBLANES, STRIP), jnp.float32),
        ]
        + row_scratch(n),
        cost_estimate=cost(arrays[0], 10),
        compiler_params=params_of(8 << 20, 2 * bit + 2),
    )(*arrays)


def store_all(*arrays):
    return pl.pallas_call(
        whole_store_kernel,
        in_specs=[VMEM] * 4,
        out_specs=[HBM] * 4,
        out_shape=[shape(*a.shape) for a in arrays[:3]] + [shape(1, 1)],
        scratch_shapes=[pltpu.SemaphoreType.DMA((4,)), pltpu.VMEM((1, 1), jnp.float32)],
        compiler_params=params_of(1 << 20),
    )(*arrays)


def store_early(bit, chunks, mine, shared, peer, part):
    return pl.pallas_call(
        partial(early_store_kernel, bit, chunks),
        in_specs=[VMEM] * 4,
        out_specs=[HBM] * 3 + [VMEM],
        out_shape=[shape(*mine.shape)] * 3 + [pltpu.VMEM(part.shape, jnp.float32)],
        scratch_shapes=[pltpu.SemaphoreType.DMA((2, chunks)), pltpu.SemaphoreType.DMA],
        compiler_params=params_of(1 << 20),
    )(mine, shared, peer, part)


def store_late(bit, chunks, mine, peer, mine_tail, peer_tail, gap, mine_hbm, peer_hbm):
    return pl.pallas_call(
        partial(late_store_kernel, bit, chunks),
        in_specs=[VMEM] * 5 + [HBM] * 2,
        out_specs=[HBM] * 3,
        out_shape=[shape(*mine_hbm.shape)] * 2 + [shape(1, 1)],
        input_output_aliases={5: 0, 6: 1},
        scratch_shapes=[
            pltpu.SemaphoreType.DMA((2, chunks)),
            pltpu.SemaphoreType.DMA,
            pltpu.VMEM((1, 1), jnp.float32),
        ],
        compiler_params=params_of(1 << 20),
    )(mine, peer, mine_tail, peer_tail, gap, mine_hbm, peer_hbm)


def round_of(bit, params, public, peer_public):
    if bit == 0:
        return store_all(*open_round(bit, True, params, public, peer_public))
    mine, shared, peer, coded, scale, part = open_round(bit, False, params, public, peer_public)
    chunks = coded.shape[0]
    params_new, public_new, peer_new, part = store_early(bit, chunks, mine, shared, peer, part)
    *tails, gap = close_round(bit, chunks, mine, shared, peer, coded, scale, part)
    params_new, peer_new, gap = store_late(bit, chunks, mine, peer, *tails, gap, params_new, peer_new)
    return params_new, public_new, peer_new, gap


def shards(params, public, peer_public, round_index):
    n = lax.axis_size("node")
    bit_count = n.bit_length() - 1
    chosen_bit = lax.rem(round_index[0], jnp.int32(bit_count))
    branches = [partial(round_of, bit) for bit in range(bit_count)]
    params_new, public_new, peer_new, gap = lax.switch(
        chosen_bit, branches, params, public, peer_public
    )
    return (params_new, public_new, peer_new, gap[0, 0])


def solution(mesh):
    in_specs = (P("node", None), P("node", None), P("node", None), P())
    out_specs = (P("node", None), P("node", None), P("node", None), P())
    return jax.shard_map(shards, mesh=mesh, in_specs=in_specs, out_specs=out_specs, check_vma=False)
```
